32 devices in a mesh: row: 4 (over z), col: 8 (over y, x, core).
Axes of the slice: x: 2, y: 2, z: 4, core: 2. Of those that a mesh axis runs over, the one named last changes fastest.
Arguments:
- src_field: bfloat16 [64, 1048576], P(None, ('row', 'col')), may hold values from 0.5 to 2
- src_area: float32 [1048576], P(('row', 'col')), may hold values from 0.3 to 3
- tgt_area: float32 [262144], P(('row', 'col')), may hold values from 0.3 to 3
- weights: bfloat16 [12288, 128, 128], P(('row', 'col')), may hold values from 0 to 0.0025939941
- send_index: int32 [32, 32, 2], P(('row', 'col')), may hold values from -1 to 255, as said below
- pair_slot: int32 [12288], P(('row', 'col')), may hold values from 0 to 63, as said below
- pair_target: int32 [12288], P(('row', 'col')), may hold values from 0 to 63, as said below
Outputs:
- target_field: float32 [64, 262144], P(None, ('row', 'col'))
The draws below stay inside these ranges and needn't reach their ends.
Inputs may be any that keep to these rules, and one draw needn't show every extreme that they name: `send_index`: in each [s, r] the live entries (not -1) come first and there are 1 to 2 of them; every sender sends to every receiver; for each receiver some sender fills all 2 slots. `pair_slot`: each pair of device r names a live slot of what device r receives; every live slot is named by some pair of device r. `pair_target`: every local target block of a device is named by some pair of that device.
All inputs are finite; a program needn't handle non-finite values.
Results may differ from the reference program's by a relative error of at most 0.0003.
Values may be sent and summed in bfloat16 or wider, within the bound.
A program may use at most 128 MiB of HBM per device.

```python
import math
import jax
import jax.numpy as jnp
from jax import lax

VARS = 8
LEV = 8
BLK = 128
CAP = 2
SB_DEV = 256
TB_DEV = 64
PAIRS_DEV = 384
NEAR = 32
NSB = 8192
NTB = 2048
PAIRS = 12288
N_ROW = 4
N_COL = 8


def routing(key):
    peer_count = N_ROW * N_COL
    base = jax.random.fold_in(key, 7)
    offsets = jnp.arange(NEAR, dtype=jnp.int32)
    receivers = jnp.arange(peer_count, dtype=jnp.int32)
    senders_of = (receivers[:, None] + offsets[None, :]) % peer_count
    near_counts = jax.random.randint(jax.random.fold_in(base, 1), (peer_count, NEAR), 1, CAP + 1)
    full_near = jax.random.randint(jax.random.fold_in(base, 2), (peer_count,), 0, NEAR)
    near_counts = jnp.where(jnp.arange(NEAR)[None, :] == full_near[:, None], CAP, near_counts)
    receiver_grid = jnp.broadcast_to(receivers[:, None], (peer_count, NEAR))
    counts = jnp.zeros((peer_count, peer_count), jnp.int32).at[senders_of, receiver_grid].set(near_counts)
    local_pick = jax.random.randint(jax.random.fold_in(base, 3), (peer_count, peer_count, CAP), 0, SB_DEV)
    alive_mask = jnp.arange(CAP)[None, None, :] < counts[:, :, None]
    send_index = jnp.where(alive_mask, local_pick, -1).astype(jnp.int32)
    position = jnp.arange(PAIRS_DEV, dtype=jnp.int32)
    near_pos = jnp.minimum(position // CAP, NEAR - 1)
    slot_pos = position % CAP
    first_sender = senders_of[:, near_pos]
    first_count = near_counts[:, near_pos]
    first_pick = jnp.where(slot_pos[None, :] < first_count, first_sender * CAP + slot_pos[None, :], first_sender * CAP)
    extra_near = jax.random.randint(jax.random.fold_in(base, 4), (peer_count, PAIRS_DEV), 0, NEAR)
    extra_raw = jax.random.randint(jax.random.fold_in(base, 6), (peer_count, PAIRS_DEV), 0, CAP)
    extra_sender = jnp.take_along_axis(senders_of, extra_near, axis=1)
    extra_count = jnp.take_along_axis(near_counts, extra_near, axis=1)
    extra_pick = extra_sender * CAP + extra_raw % extra_count
    slots_all = jnp.where((position < NEAR * CAP)[None, :], first_pick, extra_pick)
    targets_all = jnp.broadcast_to((position % TB_DEV)[None, :], (peer_count, PAIRS_DEV))
    shuffle = jax.vmap(lambda sub: jax.random.permutation(sub, PAIRS_DEV))(jax.random.split(jax.random.fold_in(base, 5), peer_count))
    pair_slot = jnp.take_along_axis(slots_all, shuffle, axis=1).reshape(-1).astype(jnp.int32)
    pair_target = jnp.take_along_axis(targets_all, shuffle, axis=1).reshape(-1).astype(jnp.int32)
    return (send_index, pair_slot, pair_target)


def draw_send_index(key, part):
    return routing(key)[0]


def draw_pair_slot(key, part):
    return routing(key)[1]


def draw_pair_target(key, part):
    return routing(key)[2]


def shard_levels(stream_key, dims, cuts, smallest, largest):
    def one(dim, blocks):
        heights = jax.random.uniform(jax.random.fold_in(jax.random.fold_in(stream_key, 6), dim), (blocks,), jnp.float32, smallest / len(cuts), largest / len(cuts))
        return jnp.repeat(jnp.exp(heights), dims[dim] // blocks).reshape((-1,) + (1,) * (len(dims) - dim - 1))

    gain = one(*cuts[0])
    for cut in cuts[1:]:
        gain = gain * one(*cut)
    return gain


def setup_inputs(seed: int = 0) -> dict:
    splits = jax.random.split(jax.random.key(seed), 8)
    src_field = jnp.clip(0.5 + 1.5 * jax.random.uniform(splits[0], (VARS * LEV, NSB * BLK), jnp.float32) ** shard_levels(splits[0], (VARS * LEV, NSB * BLK), ((1, 32),), -0.2, 0.2), 0.5, 2.0).astype(jnp.bfloat16)
    src_area = jnp.clip(jnp.exp(math.log(3.0) - 2.3025851 * jax.random.uniform(splits[1], (NSB * BLK,), jnp.float32) ** shard_levels(splits[1], (NSB * BLK,), ((0, 32),), -0.2, 0.2)), 0.3, 3.0)
    tgt_area = jnp.clip(jnp.exp(math.log(3.0) - 2.3025851 * jax.random.uniform(splits[2], (NTB * BLK,), jnp.float32) ** shard_levels(splits[2], (NTB * BLK,), ((0, 32),), -0.2, 0.2)), 0.3, 3.0)
    weights = jnp.clip(0.0025939941 * jax.random.uniform(splits[3], (PAIRS, BLK, BLK), jnp.float32) ** shard_levels(splits[3], (PAIRS, BLK, BLK), ((0, 32),), -0.2, 0.2), 0.0, 0.0025939941).astype(jnp.bfloat16)
    send_index = draw_send_index(jax.random.fold_in(splits[7], 71), 0)
    pair_slot = draw_pair_slot(jax.random.fold_in(splits[7], 71), 0)
    pair_target = draw_pair_target(jax.random.fold_in(splits[7], 71), 0)
    return {"src_field": src_field, "src_area": src_area, "tgt_area": tgt_area, "weights": weights, "send_index": send_index, "pair_slot": pair_slot, "pair_target": pair_target}


def reference(src_field, src_area, tgt_area, weights, send_index, pair_slot, pair_target):
    peer_count = N_ROW * N_COL
    columns = VARS * LEV
    blocks = src_field.reshape(columns, peer_count * SB_DEV, BLK)

    def per_receiver(receiver):
        slot_ids = lax.dynamic_slice_in_dim(pair_slot, receiver * PAIRS_DEV, PAIRS_DEV)
        targets = lax.dynamic_slice_in_dim(pair_target, receiver * PAIRS_DEV, PAIRS_DEV)
        tiles = lax.dynamic_slice_in_dim(weights, receiver * PAIRS_DEV, PAIRS_DEV, 0)
        sender = slot_ids // CAP
        slot_pos = slot_ids % CAP
        local_ids = send_index[sender, receiver, slot_pos]
        global_ids = (sender * SB_DEV + local_ids).astype(jnp.int32)
        picked = jnp.take(blocks, global_ids, axis=1)
        products = jnp.einsum('cps,pst->pct', picked.astype(jnp.float32), tiles.astype(jnp.float32), precision=lax.Precision.HIGHEST)
        return jax.ops.segment_sum(products, targets, num_segments=TB_DEV)

    regridded = lax.map(per_receiver, jnp.arange(peer_count, dtype=jnp.int32))
    regridded = jnp.transpose(regridded, (2, 0, 1, 3)).reshape(columns, peer_count * TB_DEV * BLK)
    source_mass = jnp.sum(src_field.astype(jnp.float32) * src_area[None, :], axis=1)
    target_mass = jnp.sum(regridded * tgt_area[None, :], axis=1)
    return regridded * (source_mass / target_mass)[:, None]
```

```python
import functools

import jax
import jax.numpy as jnp
from jax import lax
from jax.experimental import pallas as pl
from jax.experimental.pallas import tpu as pltpu
from jax.sharding import PartitionSpec as P

MESH = pl.DeviceIdType.MESH
LANES = 128


def lanes_of(column):
    total = jnp.sum(column, axis=1, keepdims=True)
    rows = lax.broadcasted_iota(jnp.int32, column.shape, 0)
    lanes = lax.broadcasted_iota(jnp.int32, column.shape, 1)
    return jnp.sum(jnp.where(rows == lanes, total, 0.0), axis=0, keepdims=True)


def place(cols):
    me = lax.axis_index("row") * cols + lax.axis_index("col")
    return me


def greet(n, cols, me):
    barrier = pltpu.get_barrier_semaphore()

    def hello(step, carry):
        peer = lax.rem(me + step, n)
        pl.semaphore_signal(barrier, inc=1, device_id=(peer // cols, lax.rem(peer, cols)), device_id_type=MESH)
        return carry

    lax.fori_loop(1, n, hello, 0)
    return barrier


def exchange_kernel(n, cols, send_ref, area_ref, src_ref, inbound_ref, mass_ref, src, outbound, load_sem, keep_sem, send_sem, recv_sem):
    me = place(cols)
    capacity, columns, block = outbound.shape[1:]

    def load(index, carry):
        cells = pl.ds(pl.multiple_of(index * block, block), block)
        pltpu.make_async_copy(src_ref.at[:, cells], src.at[index], load_sem).start()
        return carry

    lax.fori_loop(0, src.shape[0], load, 0, unroll=8)
    barrier = greet(n, cols, me)
    pltpu.make_async_copy(src, src, load_sem).wait()

    def gather(peer, carry):
        for slot in range(capacity):
            pick = jnp.maximum(send_ref[peer * capacity + slot], 0)
            outbound[peer, slot] = src[pick]
        return carry

    lax.fori_loop(0, n, gather, 0)
    pl.semaphore_wait(barrier, n - 1)

    def copy_to(step):
        peer = lax.rem(me + step, n)
        return pltpu.make_async_remote_copy(
            src_ref=outbound.at[peer],
            dst_ref=inbound_ref.at[me],
            send_sem=send_sem.at[step],
            recv_sem=recv_sem.at[step],
            device_id=(peer // cols, lax.rem(peer, cols)),
            device_id_type=MESH,
        )

    def send(step, carry):
        copy_to(step).start()
        return carry

    lax.fori_loop(1, n, send, 0)
    keep = pltpu.make_async_copy(outbound.at[me], inbound_ref.at[me], keep_sem)
    keep.start()

    def add(step, total):
        return total + src[step].astype(jnp.float32) * area_ref[pl.ds(step, 1), :]

    total = lax.fori_loop(0, area_ref.shape[0], add, jnp.zeros((columns, block), jnp.float32), unroll=8)
    mass_ref[...] = jnp.broadcast_to(lanes_of(total), mass_ref.shape)
    keep.wait()

    def finish(step, carry):
        copy_to(step).wait()
        return carry

    lax.fori_loop(1, n, finish, 0)


def exchange(n, cols, capacity, send_rows, area, src_field):
    columns, cells = src_field.shape
    block = area.shape[1]
    return pl.pallas_call(
        functools.partial(exchange_kernel, n, cols),
        out_shape=(
            jax.ShapeDtypeStruct((n, capacity, columns, block), jnp.bfloat16),
            jax.ShapeDtypeStruct((8, LANES), jnp.float32),
        ),
        in_specs=[
            pl.BlockSpec(memory_space=pltpu.SMEM),
            pl.BlockSpec(memory_space=pltpu.VMEM),
            pl.BlockSpec(memory_space=pl.ANY),
        ],
        out_specs=(pl.BlockSpec(memory_space=pl.ANY), pl.BlockSpec(memory_space=pltpu.VMEM)),
        scratch_shapes=[
            pltpu.VMEM((cells // block, columns, block), jnp.bfloat16),
            pltpu.VMEM((n, capacity, columns, block), jnp.bfloat16),
            pltpu.SemaphoreType.DMA,
            pltpu.SemaphoreType.DMA,
            pltpu.SemaphoreType.DMA((n,)),
            pltpu.SemaphoreType.DMA((n,)),
        ],
        compiler_params=pltpu.CompilerParams(collective_id=0, has_side_effects=True),
        name="exchange",
    )(send_rows, area, src_field)


def regrid_kernel(group, slot_ref, target_ref, inbound_ref, area_ref, weight_ref, out_ref, mass_ref):
    step = pl.program_id(0)
    pairs, block = weight_ref.shape[:2]
    columns = out_ref.shape[0]

    @pl.when(step == 0)
    def _():
        out_ref[...] = jnp.zeros_like(out_ref)

    @pl.loop(0, pairs // group)
    def _(outer):
        first = outer * group
        products = []
        for inner in range(group):
            slot = slot_ref[step * pairs + first + inner]
            products.append(jnp.dot(inbound_ref[slot], weight_ref[first + inner], preferred_element_type=jnp.float32))
        for inner in range(group):
            target = target_ref[step * pairs + first + inner]
            cells = pl.ds(pl.multiple_of(target * block, block), block)
            out_ref[:, cells] += products[inner]

    @pl.when(step == pl.num_programs(0) - 1)
    def _():
        def add(index, total):
            return total + out_ref[:, pl.ds(pl.multiple_of(index * block, block), block)] * area_ref[pl.ds(index, 1), :]

        total = lax.fori_loop(0, area_ref.shape[0], add, jnp.zeros((columns, block), jnp.float32), unroll=8)
        mass_ref[...] = jnp.broadcast_to(lanes_of(total), mass_ref.shape)


def regrid(inbound, area, weights, pair_slot, pair_target):
    slots, columns, block = inbound.shape
    pairs = weights.shape[0]
    targets = area.shape[0]
    step = 32
    whole = lambda *shape: pl.BlockSpec(shape, lambda i, *_: (0,) * len(shape))
    return pl.pallas_call(
        functools.partial(regrid_kernel, 4),
        out_shape=(
            jax.ShapeDtypeStruct((columns, targets * block), jnp.float32),
            jax.ShapeDtypeStruct((8, LANES), jnp.float32),
        ),
        grid_spec=pltpu.PrefetchScalarGridSpec(
            num_scalar_prefetch=2,
            grid=(pairs // step,),
            in_specs=[
                whole(slots, columns, block),
                whole(targets, block),
                pl.BlockSpec((step, block, block), lambda i, *_: (i, 0, 0)),
            ],
            out_specs=(whole(columns, targets * block), whole(8, LANES)),
        ),
        name="regrid",
    )(pair_slot, pair_target, inbound, area, weights)


def mass_kernel(n, cols, source_ref, target_ref, scale_ref, own, seen, send_sem, recv_sem):
    me = place(cols)
    barrier = greet(n, cols, me)
    rows = lax.broadcasted_iota(jnp.int32, own.shape, 0)
    own[...] = jnp.where(rows == 0, source_ref[...], target_ref[...])
    pl.semaphore_wait(barrier, n - 1)

    def copy_to(step):
        peer = lax.rem(me + step, n)
        return pltpu.make_async_remote_copy(
            src_ref=own,
            dst_ref=seen.at[step],
            send_sem=send_sem.at[step],
            recv_sem=recv_sem.at[step],
            device_id=(peer // cols, lax.rem(peer, cols)),
            device_id_type=MESH,
        )

    def send(step, carry):
        copy_to(step).start()
        return carry

    def finish(step, total):
        copy_to(step).wait()
        return total + seen[step]

    lax.fori_loop(1, n, send, 0)
    total = lax.fori_loop(1, n, finish, own[...])
    scale_ref[...] = jnp.broadcast_to(total[0:1] / total[1:2], scale_ref.shape)


def scales(n, cols, source, target):
    return pl.pallas_call(
        functools.partial(mass_kernel, n, cols),
        out_shape=jax.ShapeDtypeStruct((8, LANES), jnp.float32),
        in_specs=[pl.BlockSpec(memory_space=pltpu.VMEM)] * 2,
        out_specs=pl.BlockSpec(memory_space=pltpu.VMEM),
        scratch_shapes=[
            pltpu.VMEM((8, LANES), jnp.float32),
            pltpu.VMEM((n, 8, LANES), jnp.float32),
            pltpu.SemaphoreType.DMA((n,)),
            pltpu.SemaphoreType.DMA((n,)),
        ],
        compiler_params=pltpu.CompilerParams(collective_id=1, has_side_effects=True),
        name="masses",
    )(source, target)


def shards(n, cols, src_field, src_area, tgt_area, weights, send_index, pair_slot, pair_target):
    columns, cell_count = src_field.shape
    block = weights.shape[1]
    capacity = send_index.shape[2]
    inbound, source = exchange(n, cols, capacity, send_index.reshape(-1), src_area.reshape(-1, block), src_field)
    regridded, target = regrid(inbound.reshape(n * capacity, columns, block), tgt_area.reshape(-1, block), weights, pair_slot, pair_target)
    scale = scales(n, cols, source, target)
    return regridded * scale[0, :columns][:, None]


def solution(mesh):
    rows, cols = mesh.shape["row"], mesh.shape["col"]
    in_specs = (
        P(None, ("row", "col")),
        P(("row", "col")),
        P(("row", "col")),
        P(("row", "col"), None, None),
        P(("row", "col"), None, None),
        P(("row", "col")),
        P(("row", "col")),
    )
    out_specs = P(None, ("row", "col"))
    body = functools.partial(shards, rows * cols, cols)
    return jax.shard_map(body, mesh=mesh, in_specs=in_specs, out_specs=out_specs, check_vma=False)
```

```python
import functools

import jax
import jax.numpy as jnp
from jax import lax
from jax.experimental import pallas as pl
from jax.experimental.pallas import tpu as pltpu
from jax.sharding import PartitionSpec as P

MESH = pl.DeviceIdType.MESH
LANES = 128


def lanes_of(column):
    total = jnp.sum(column, axis=1, keepdims=True)
    rows = lax.broadcasted_iota(jnp.int32, column.shape, 0)
    lanes = lax.broadcasted_iota(jnp.int32, column.shape, 1)
    return jnp.sum(jnp.where(rows == lanes, total, 0.0), axis=0, keepdims=True)


def place(cols):
    me = lax.axis_index("row") * cols + lax.axis_index("col")
    return me


def greet(n, cols, me):
    barrier = pltpu.get_barrier_semaphore()

    def hello(step, carry):
        peer = lax.rem(me + step, n)
        pl.semaphore_signal(barrier, inc=1, device_id=(peer // cols, lax.rem(peer, cols)), device_id_type=MESH)
        return carry

    lax.fori_loop(1, n, hello, 0)
    return barrier


def exchange_kernel(
    n, cols, cuts, send_ref, slot_ref, target_ref, slots_ref, source_area_ref, target_area_ref, src_ref, weight_ref,
    inbound_ref, scale_ref,
    src, outbound, weights, asked, wanted, part, own, seen,
    load_sem, weight_sem, keep_sem, send_sem, recv_sem, ask_send, ask_recv, mass_send, mass_recv,
):
    me = place(cols)
    capacity, columns, block = outbound.shape[1:]
    pairs = weight_ref.shape[0]
    chunks = weight_sem.shape[0]
    chunk = pairs // chunks

    def load(index, carry):
        cells = pl.ds(pl.multiple_of(index * block, block), block)
        pltpu.make_async_copy(src_ref.at[:, cells], src.at[index], load_sem).start()
        return carry

    def fetch(index):
        piece = pl.ds(index * chunk, chunk)
        return pltpu.make_async_copy(weight_ref.at[piece], weights.at[piece], weight_sem.at[index])

    lax.fori_loop(0, src.shape[0], load, 0, unroll=8)
    barrier = greet(n, cols, me)
    pltpu.make_async_copy(src, src, load_sem).wait()
    for index in range(chunks):
        fetch(index).start()

    def gather(peer, carry):
        for slot in range(capacity):
            outbound[peer, slot] = src[jnp.maximum(send_ref[slot, peer], 0)]
        return carry

    lax.fori_loop(0, n, gather, 0)
    pl.semaphore_wait(barrier, n - 1)

    def to_peer(step, source, target, sent, received):
        peer = lax.rem(me + step, n)
        return pltpu.make_async_remote_copy(
            src_ref=source(peer),
            dst_ref=target,
            send_sem=sent.at[step],
            recv_sem=received.at[step],
            device_id=(peer // cols, lax.rem(peer, cols)),
            device_id_type=MESH,
        )

    def blocks(step):
        return to_peer(step, lambda peer: outbound.at[peer], inbound_ref.at[me], send_sem, recv_sem)

    def asks(step):
        return to_peer(step, lambda peer: wanted.at[peer], asked.at[step], ask_send, ask_recv)

    def masses(step):
        return to_peer(step, lambda peer: own, seen.at[step], mass_send, mass_recv)

    def start(copy, low, high):
        def one(step, carry):
            copy(step).start()
            return carry

        lax.fori_loop(low, high, one, 0)

    start(blocks, 1, cuts[0])
    keep = pltpu.make_async_copy(outbound.at[me], inbound_ref.at[me], keep_sem)
    keep.start()

    group = 8

    def fold(index, carry):
        for inner in range(group):
            j = index * group + inner
            area = target_area_ref[target_ref[j]]
            high = area.astype(jnp.bfloat16)
            rest = area - high.astype(jnp.float32)
            middle = rest.astype(jnp.bfloat16)
            low = (rest - middle.astype(jnp.float32)).astype(jnp.bfloat16)
            terms = jnp.concatenate([high, middle, low], axis=0)
            sums = lax.dot_general(terms, weights[j], (((1,), (1,)), ((), ())), preferred_element_type=jnp.float32)
            part[pl.ds(j, 1), :] = sums[0:1] + sums[1:2] + sums[2:3]
        return carry

    for index in range(chunks):
        fetch(index).wait()
        lax.fori_loop(index * chunk // group, (index + 1) * chunk // group, fold, 0)

    sublanes = wanted.shape[1]
    rows = lax.broadcasted_iota(jnp.int32, (n * sublanes, pairs), 0)
    peer_of, slot_of = rows // sublanes, rows % sublanes
    names = jnp.where(slot_of < capacity, peer_of * capacity + slot_of, -1)
    chosen = jnp.where(names == slots_ref[...], 1.0, 0.0)
    sums = jnp.dot(chosen, part[...], precision=lax.Precision.HIGHEST, preferred_element_type=jnp.float32)
    wanted[...] = sums.reshape(wanted.shape)

    start(asks, 1, n)
    start(blocks, cuts[0], cuts[1])

    def add(index, total):
        return total + src[index].astype(jnp.float32) * source_area_ref[pl.ds(index, 1), :]

    zero = jnp.zeros((columns, block), jnp.float32)
    source = lanes_of(lax.fori_loop(0, src.shape[0], add, zero, unroll=8))

    def weigh(peer, share, total):
        for slot in range(capacity):
            total = total + outbound[peer, slot].astype(jnp.float32) * share[slot : slot + 1]
        return total

    def arrived(step, total):
        asks(step).wait()
        return weigh(lax.rem(me + n - step, n), asked[step], total)

    target = lanes_of(lax.fori_loop(1, n, arrived, weigh(me, wanted[me], zero)))
    rows = lax.broadcasted_iota(jnp.int32, own.shape, 0)
    own[...] = jnp.where(rows == 0, source, target)
    start(masses, 1, n)
    start(blocks, cuts[1], n)

    def collect(step, total):
        masses(step).wait()
        return total + seen[step]

    total = lax.fori_loop(1, n, collect, own[...])
    ratio = jnp.broadcast_to(total[0:1] / total[1:2], (columns, block))
    diagonal = lax.broadcasted_iota(jnp.int32, ratio.shape, 0) == lax.broadcasted_iota(jnp.int32, ratio.shape, 1)
    scale_ref[...] = jnp.broadcast_to(jnp.sum(jnp.where(diagonal, ratio, 0.0), axis=1, keepdims=True), ratio.shape)
    keep.wait()

    def finish(step, carry):
        blocks(step).wait()
        return carry

    lax.fori_loop(1, n, finish, 0)


def exchange(n, cols, send_rows, pair_slot, pair_target, source_area, target_area, src_field, weights):
    columns, cells = src_field.shape
    block = source_area.shape[1]
    capacity = send_rows.shape[0]
    pairs = weights.shape[0]
    cuts = (max(n * 4 // 10, 1), max(n * 7 // 10, 1))
    vmem = pl.BlockSpec(memory_space=pltpu.VMEM)
    smem = pl.BlockSpec(memory_space=pltpu.SMEM)
    hbm = pl.BlockSpec(memory_space=pl.ANY)
    per_peer = pltpu.SemaphoreType.DMA((n,))
    return pl.pallas_call(
        functools.partial(exchange_kernel, n, cols, cuts),
        out_shape=(
            jax.ShapeDtypeStruct((n, capacity, columns, block), jnp.bfloat16),
            jax.ShapeDtypeStruct((columns, block), jnp.float32),
        ),
        in_specs=[smem, smem, smem, vmem, vmem, vmem, hbm, hbm],
        out_specs=(hbm, vmem),
        scratch_shapes=[
            pltpu.VMEM((cells // block, columns, block), jnp.bfloat16),
            pltpu.VMEM((n, capacity, columns, block), jnp.bfloat16),
            pltpu.VMEM(weights.shape, jnp.bfloat16),
            pltpu.VMEM((n, 8, block), jnp.float32),
            pltpu.VMEM((n, 8, block), jnp.float32),
            pltpu.VMEM((pairs, block), jnp.float32),
            pltpu.VMEM((8, block), jnp.float32),
            pltpu.VMEM((n, 8, block), jnp.float32),
            pltpu.SemaphoreType.DMA,
            pltpu.SemaphoreType.DMA((4,)),
            pltpu.SemaphoreType.DMA,
        ]
        + [per_peer] * 6,
        compiler_params=pltpu.CompilerParams(collective_id=0, has_side_effects=True),
        name="exchange",
    )(send_rows, pair_slot, pair_target, pair_slot.reshape(1, pairs), source_area, target_area, src_field, weights)


def regrid_kernel(lag, slot_ref, target_ref, inbound_ref, scale_ref, weight_ref, out_ref):
    step = pl.program_id(0)
    group, block = weight_ref.shape[:2]
    products = {}

    @pl.when(step == 0)
    def _():
        out_ref[...] = jnp.zeros_like(out_ref)

    def cells_of(target):
        return pl.ds(pl.multiple_of(target * block, block), block)

    for inner in range(group + lag):
        if inner < group:
            slot = slot_ref[step * group + inner]
            products[inner] = jnp.dot(inbound_ref[slot], weight_ref[inner], preferred_element_type=jnp.float32)
        if inner >= lag:
            cells = cells_of(target_ref[step * group + inner - lag])
            out_ref[:, cells] += products.pop(inner - lag)

    @pl.when(step == pl.num_programs(0) - 1)
    def _():
        def fix(index, carry):
            out_ref[:, cells_of(index)] = out_ref[:, cells_of(index)] * scale_ref[...]
            return carry

        lax.fori_loop(0, out_ref.shape[1] // block, fix, 0, unroll=8)


def regrid(inbound, scale, weights, pair_slot, pair_target, targets):
    slots, columns, block = inbound.shape
    pairs = weights.shape[0]
    group = next(g for g in (48, 32, 16, 8, 4, 2, 1) if pairs % g == 0)
    whole = lambda *shape: pl.BlockSpec(shape, lambda i, *_: (0,) * len(shape))
    return pl.pallas_call(
        functools.partial(regrid_kernel, 6),
        out_shape=jax.ShapeDtypeStruct((columns, targets * block), jnp.float32),
        grid_spec=pltpu.PrefetchScalarGridSpec(
            num_scalar_prefetch=2,
            grid=(pairs // group,),
            in_specs=[
                whole(slots, columns, block),
                whole(columns, block),
                pl.BlockSpec((group, block, block), lambda i, *_: (i, 0, 0)),
            ],
            out_specs=whole(columns, targets * block),
        ),
        name="regrid",
    )(pair_slot, pair_target, inbound, scale, weights)


def shards(n, cols, src_field, src_area, tgt_area, weights, send_index, pair_slot, pair_target):
    columns, cell_count = src_field.shape
    block = weights.shape[1]
    targets = tgt_area.shape[0] // block
    inbound, scale = exchange(
        n, cols, send_index[0].T, pair_slot, pair_target,
        src_area.reshape(-1, block), tgt_area.reshape(targets, 1, block), src_field, weights,
    )
    return regrid(inbound.reshape(-1, columns, block), scale, weights, pair_slot, pair_target, targets)


def solution(mesh):
    rows, cols = mesh.shape["row"], mesh.shape["col"]
    in_specs = (
        P(None, ("row", "col")),
        P(("row", "col")),
        P(("row", "col")),
        P(("row", "col"), None, None),
        P(("row", "col"), None, None),
        P(("row", "col")),
        P(("row", "col")),
    )
    out_specs = P(None, ("row", "col"))
    body = functools.partial(shards, rows * cols, cols)
    return jax.shard_map(body, mesh=mesh, in_specs=in_specs, out_specs=out_specs, check_vma=False)
```

```python
import functools

import jax
import jax.numpy as jnp
from jax import lax
from jax.experimental import pallas as pl
from jax.experimental.pallas import tpu as pltpu
from jax.sharding import PartitionSpec as P

MESH = pl.DeviceIdType.MESH
LANES = 128


def lanes_of(column):
    total = jnp.sum(column, axis=1, keepdims=True)
    rows = lax.broadcasted_iota(jnp.int32, column.shape, 0)
    lanes = lax.broadcasted_iota(jnp.int32, column.shape, 1)
    return jnp.sum(jnp.where(rows == lanes, total, 0.0), axis=0, keepdims=True)


def place(cols):
    me = lax.axis_index("row") * cols + lax.axis_index("col")
    return me


def greet(n, cols, me):
    barrier = pltpu.get_barrier_semaphore()

    def hello(step, carry):
        peer = lax.rem(me + step, n)
        pl.semaphore_signal(barrier, inc=1, device_id=(peer // cols, lax.rem(peer, cols)), device_id_type=MESH)
        return carry

    lax.fori_loop(1, n, hello, 0)
    return barrier


def split(value):
    high = value.astype(jnp.bfloat16)
    rest = value - high.astype(jnp.float32)
    middle = rest.astype(jnp.bfloat16)
    return high, middle, (rest - middle.astype(jnp.float32)).astype(jnp.bfloat16)


def exchange_kernel(
    n, cols, send_ref, slot_ref, target_ref, slots_ref, source_area_ref, target_area_ref, src_ref, weight_ref,
    inbound_ref, scale_ref,
    src, outbound, weights, part, shares, own, seen,
    load_sem, weight_sem, keep_sem, send_sem, recv_sem, mass_send, mass_recv,
):
    me = place(cols)
    capacity, columns, block = outbound.shape[1:]
    pairs = weight_ref.shape[0]
    chunks = weight_sem.shape[0]
    chunk = pairs // chunks

    def load(index, carry):
        cells = pl.ds(pl.multiple_of(index * block, block), block)
        pltpu.make_async_copy(src_ref.at[:, cells], src.at[index], load_sem).start()
        return carry

    def fetch(index):
        piece = pl.ds(index * chunk, chunk)
        return pltpu.make_async_copy(weight_ref.at[piece], weights.at[piece], weight_sem.at[index])

    lax.fori_loop(0, src.shape[0], load, 0, unroll=8)
    barrier = greet(n, cols, me)
    pltpu.make_async_copy(src, src, load_sem).wait()
    for index in range(chunks):
        fetch(index).start()

    def gather(peer, carry):
        for slot in range(capacity):
            outbound[peer, slot] = src[jnp.maximum(send_ref[slot, peer], 0)]
        return carry

    lax.fori_loop(0, n, gather, 0)
    pl.semaphore_wait(barrier, n - 1)

    def blocks(step):
        peer = lax.rem(me + step, n)
        return pltpu.make_async_remote_copy(
            src_ref=outbound.at[peer],
            dst_ref=inbound_ref.at[me],
            send_sem=send_sem.at[step],
            recv_sem=recv_sem.at[step],
            device_id=(peer // cols, lax.rem(peer, cols)),
            device_id_type=MESH,
        )

    def send(step, carry):
        blocks(step).start()
        return carry

    lax.fori_loop(1, n, send, 0)
    keep = pltpu.make_async_copy(outbound.at[me], inbound_ref.at[me], keep_sem)
    keep.start()

    group = max(g for g in (16, 8, 4, 2, 1) if chunk % g == 0)
    row = lax.broadcasted_iota(jnp.int32, (group, block), 0)

    def fold(index, carry):
        first = index * group
        area = jnp.concatenate([target_area_ref[target_ref[first + inner]] for inner in range(group)], axis=0)
        tiles = weights[pl.ds(first, group)].reshape(group * block, block)
        terms = jnp.concatenate(split(area), axis=0)
        sums = lax.dot_general(terms, tiles, (((1,), (1,)), ((), ())), preferred_element_type=jnp.float32)
        sums = sums[:group] + sums[group : 2 * group] + sums[2 * group :]
        own_sums = sums[:, :block]
        for inner in range(1, group):
            own_sums = jnp.where(row == inner, sums[:, inner * block : (inner + 1) * block], own_sums)
        part[pl.ds(pl.multiple_of(first, group), group), :] = own_sums
        return carry

    for index in range(chunks):
        fetch(index).wait()
        lax.fori_loop(index * chunk // group, (index + 1) * chunk // group, fold, 0)

    sublanes = shares.shape[1]
    rows = lax.broadcasted_iota(jnp.int32, (n * sublanes, pairs), 0)
    peer_of, slot_of = rows // sublanes, rows % sublanes
    names = jnp.where(slot_of < capacity, peer_of * capacity + slot_of, -1)
    chosen = jnp.where(names == slots_ref[...].reshape(1, pairs), 1.0, 0.0).astype(jnp.bfloat16)
    sums = jnp.dot(chosen, jnp.concatenate(split(part[...]), axis=1), preferred_element_type=jnp.float32)
    sums = sums[:, :block] + sums[:, block : 2 * block] + sums[:, 2 * block :]
    shares[...] = sums.reshape(shares.shape)

    def add(index, total):
        return total + src[index].astype(jnp.float32) * source_area_ref[pl.ds(index, 1), :]

    zero = jnp.zeros((columns, block), jnp.float32)
    source = lanes_of(lax.fori_loop(0, src.shape[0], add, zero, unroll=8))

    def weigh(peer, held, total):
        share = shares[peer]
        for slot in range(capacity):
            total = total + held[peer, slot].astype(jnp.float32) * share[slot : slot + 1]
        return total

    def arrived(step, total):
        blocks(step).wait_recv()
        return weigh(lax.rem(me + n - step, n), inbound_ref, total)

    target = lanes_of(lax.fori_loop(1, n, arrived, weigh(me, outbound, zero)))
    rows = lax.broadcasted_iota(jnp.int32, own.shape[1:], 0)
    total = jnp.where(rows == 0, source, target)
    row, col = lax.axis_index("row"), lax.axis_index("col")
    for stage, size in enumerate((cols, n // cols)):
        own[stage] = total

        def masses(step):
            peer = (row, lax.rem(col + step, size)) if stage == 0 else (lax.rem(row + step, size), col)
            return pltpu.make_async_remote_copy(
                src_ref=own.at[stage],
                dst_ref=seen.at[stage, step],
                send_sem=mass_send.at[stage, step],
                recv_sem=mass_recv.at[stage, step],
                device_id=peer,
                device_id_type=MESH,
            )

        for step in range(1, size):
            masses(step).start()
        for step in range(1, size):
            masses(step).wait()
            total = total + seen[stage, step]

    ratio = jnp.broadcast_to(total[0:1] / total[1:2], (columns, block))
    diagonal = lax.broadcasted_iota(jnp.int32, ratio.shape, 0) == lax.broadcasted_iota(jnp.int32, ratio.shape, 1)
    scale_ref[...] = jnp.broadcast_to(jnp.sum(jnp.where(diagonal, ratio, 0.0), axis=1, keepdims=True), ratio.shape)
    keep.wait()

    def finish(step, carry):
        blocks(step).wait_send()
        return carry

    lax.fori_loop(1, n, finish, 0)


def exchange(n, cols, send_rows, pair_slot, pair_target, source_area, target_area, src_field, weights):
    columns, cells = src_field.shape
    block = source_area.shape[1]
    capacity = send_rows.shape[0]
    pairs = weights.shape[0]
    vmem = pl.BlockSpec(memory_space=pltpu.VMEM)
    smem = pl.BlockSpec(memory_space=pltpu.SMEM)
    hbm = pl.BlockSpec(memory_space=pl.ANY)
    longest = max(cols, n // cols)
    return pl.pallas_call(
        functools.partial(exchange_kernel, n, cols),
        out_shape=(
            jax.ShapeDtypeStruct((n, capacity, columns, block), jnp.bfloat16),
            jax.ShapeDtypeStruct((columns, block), jnp.float32),
        ),
        in_specs=[smem, smem, smem, vmem, vmem, vmem, hbm, hbm],
        out_specs=(vmem, vmem),
        scratch_shapes=[
            pltpu.VMEM((cells // block, columns, block), jnp.bfloat16),
            pltpu.VMEM((n, capacity, columns, block), jnp.bfloat16),
            pltpu.VMEM(weights.shape, jnp.bfloat16),
            pltpu.VMEM((pairs, block), jnp.float32),
            pltpu.VMEM((n, 8, block), jnp.float32),
            pltpu.VMEM((2, 8, block), jnp.float32),
            pltpu.VMEM((2, longest, 8, block), jnp.float32),
            pltpu.SemaphoreType.DMA,
            pltpu.SemaphoreType.DMA((4,)),
            pltpu.SemaphoreType.DMA,
        ]
        + [pltpu.SemaphoreType.DMA((n,))] * 2
        + [pltpu.SemaphoreType.DMA((2, longest))] * 2,
        compiler_params=pltpu.CompilerParams(collective_id=0, has_side_effects=True),
        name="exchange",
    )(send_rows, pair_slot, pair_target, pair_slot, source_area, target_area, src_field, weights)


def regrid_kernel(lag, slot_ref, target_ref, inbound_ref, scale_ref, weight_ref, out_ref):
    step = pl.program_id(0)
    group, block = weight_ref.shape[:2]
    products = {}

    @pl.when(step == 0)
    def _():
        out_ref[...] = jnp.zeros_like(out_ref)

    def cells_of(target):
        return pl.ds(pl.multiple_of(target * block, block), block)

    for inner in range(group + lag):
        if inner < group:
            slot = slot_ref[step * group + inner]
            products[inner] = jnp.dot(inbound_ref[slot], weight_ref[inner], preferred_element_type=jnp.float32)
        if inner >= lag:
            cells = cells_of(target_ref[step * group + inner - lag])
            out_ref[:, cells] += products.pop(inner - lag)

    @pl.when(step == pl.num_programs(0) - 1)
    def _():
        def fix(index, carry):
            out_ref[:, cells_of(index)] = out_ref[:, cells_of(index)] * scale_ref[...]
            return carry

        lax.fori_loop(0, out_ref.shape[1] // block, fix, 0, unroll=8)


def regrid(inbound, scale, weights, pair_slot, pair_target, targets):
    slots, columns, block = inbound.shape
    pairs = weights.shape[0]
    group = next(g for g in (96, 64, 48, 32, 16, 8, 4, 2, 1) if pairs % g == 0)
    whole = lambda *shape: pl.BlockSpec(shape, lambda i, *_: (0,) * len(shape))
    return pl.pallas_call(
        functools.partial(regrid_kernel, 6),
        out_shape=jax.ShapeDtypeStruct((columns, targets * block), jnp.float32),
        grid_spec=pltpu.PrefetchScalarGridSpec(
            num_scalar_prefetch=2,
            grid=(pairs // group,),
            in_specs=[
                whole(slots, columns, block),
                whole(columns, block),
                pl.BlockSpec((group, block, block), lambda i, *_: (i, 0, 0)),
            ],
            out_specs=whole(columns, targets * block),
        ),
        name="regrid",
    )(pair_slot, pair_target, inbound, scale, weights)


def shards(n, cols, src_field, src_area, tgt_area, weights, send_index, pair_slot, pair_target):
    columns, cell_count = src_field.shape
    block = weights.shape[1]
    targets = tgt_area.shape[0] // block
    inbound, scale = exchange(
        n, cols, send_index[0].T, pair_slot, pair_target,
        src_area.reshape(-1, block), tgt_area.reshape(targets, 1, block), src_field, weights,
    )
    return regrid(inbound.reshape(-1, columns, block), scale, weights, pair_slot, pair_target, targets)


def solution(mesh):
    rows, cols = mesh.shape["row"], mesh.shape["col"]
    in_specs = (
        P(None, ("row", "col")),
        P(("row", "col")),
        P(("row", "col")),
        P(("row", "col"), None, None),
        P(("row", "col"), None, None),
        P(("row", "col")),
        P(("row", "col")),
    )
    out_specs = P(None, ("row", "col"))
    body = functools.partial(shards, rows * cols, cols)
    return jax.shard_map(body, mesh=mesh, in_specs=in_specs, out_specs=out_specs, check_vma=False)
```

```python
import functools
import math

import jax
import jax.numpy as jnp
from jax import lax
from jax.experimental import pallas as pl
from jax.experimental.pallas import tpu as pltpu
from jax.sharding import PartitionSpec as P

MESH = pl.DeviceIdType.MESH
LANES = 128


def lanes_of(column):
    total = jnp.sum(column, axis=1, keepdims=True)
    rows = lax.broadcasted_iota(jnp.int32, column.shape, 0)
    lanes = lax.broadcasted_iota(jnp.int32, column.shape, 1)
    return jnp.sum(jnp.where(rows == lanes, total, 0.0), axis=0, keepdims=True)


def place(cols):
    me = lax.axis_index("row") * cols + lax.axis_index("col")
    return me


def greet(n, cols, me):
    barrier = pltpu.get_barrier_semaphore()

    def hello(step, carry):
        peer = lax.rem(me + step, n)
        pl.semaphore_signal(barrier, inc=1, device_id=(peer // cols, lax.rem(peer, cols)), device_id_type=MESH)
        return carry

    lax.fori_loop(1, n, hello, 0)
    return barrier


def split(value):
    high = value.astype(jnp.bfloat16)
    rest = value - high.astype(jnp.float32)
    middle = rest.astype(jnp.bfloat16)
    return high, middle, (rest - middle.astype(jnp.float32)).astype(jnp.bfloat16)


def exchange_kernel(
    n, cols, send_ref, slot_ref, target_ref, slots_ref, source_area_ref, target_area_ref, src_ref, weight_ref,
    inbound_ref, scale_ref,
    src, outbound, weights, part, shares, own, seen,
    load_sem, weight_sem, keep_sem, send_sem, recv_sem, mass_send, mass_recv,
):
    me = place(cols)
    capacity, columns, block = outbound.shape[1:]
    pairs = weight_ref.shape[0]
    chunks = weight_sem.shape[0]
    chunk = pairs // chunks

    def load(index, carry):
        cells = pl.ds(pl.multiple_of(index * block, block), block)
        pltpu.make_async_copy(src_ref.at[:, cells], src.at[index], load_sem).start()
        return carry

    def fetch(index):
        piece = pl.ds(index * chunk, chunk)
        return pltpu.make_async_copy(weight_ref.at[piece], weights.at[piece], weight_sem.at[index])

    lax.fori_loop(0, src.shape[0], load, 0, unroll=8)
    barrier = greet(n, cols, me)
    pltpu.make_async_copy(src, src, load_sem).wait()
    for index in range(chunks):
        fetch(index).start()

    def gather(peer, carry):
        for slot in range(capacity):
            outbound[peer, slot] = src[jnp.maximum(send_ref[slot, peer], 0)]
        return carry

    lax.fori_loop(0, n, gather, 0)
    pl.semaphore_wait(barrier, n - 1)

    row, col = lax.axis_index("row"), lax.axis_index("col")
    steps = order(n // cols, cols)

    def blocks(step):
        down, across = steps[step]
        to_row, to_col = lax.rem(row + down, n // cols), lax.rem(col + across, cols)
        return pltpu.make_async_remote_copy(
            src_ref=outbound.at[to_row * cols + to_col],
            dst_ref=inbound_ref.at[me],
            send_sem=send_sem.at[step],
            recv_sem=recv_sem.at[step],
            device_id=(to_row, to_col),
            device_id_type=MESH,
        )

    for step in range(n - 1):
        blocks(step).start()
    keep = pltpu.make_async_copy(outbound.at[me], inbound_ref.at[me], keep_sem)
    keep.start()

    group = max(g for g in (16, 8, 4, 2, 1) if chunk % g == 0)
    place_of = lax.broadcasted_iota(jnp.int32, (group, block), 0)

    def fold(index, carry):
        first = index * group
        area = jnp.concatenate([target_area_ref[target_ref[first + inner]] for inner in range(group)], axis=0)
        tiles = weights[pl.ds(first, group)].reshape(group * block, block)
        terms = jnp.concatenate(split(area), axis=0)
        sums = lax.dot_general(terms, tiles, (((1,), (1,)), ((), ())), preferred_element_type=jnp.float32)
        sums = sums[:group] + sums[group : 2 * group] + sums[2 * group :]
        own_sums = sums[:, :block]
        for inner in range(1, group):
            own_sums = jnp.where(place_of == inner, sums[:, inner * block : (inner + 1) * block], own_sums)
        part[pl.ds(pl.multiple_of(first, group), group), :] = own_sums
        return carry

    for index in range(chunks):
        fetch(index).wait()
        lax.fori_loop(index * chunk // group, (index + 1) * chunk // group, fold, 0)

    sublanes = shares.shape[1]
    rows = lax.broadcasted_iota(jnp.int32, (n * sublanes, pairs), 0)
    peer_of, slot_of = rows // sublanes, rows % sublanes
    names = jnp.where(slot_of < capacity, peer_of * capacity + slot_of, -1)
    chosen = jnp.where(names == slots_ref[...].reshape(1, pairs), 1.0, 0.0).astype(jnp.bfloat16)
    sums = jnp.dot(chosen, jnp.concatenate(split(part[...]), axis=1), preferred_element_type=jnp.float32)
    sums = sums[:, :block] + sums[:, block : 2 * block] + sums[:, 2 * block :]
    shares[...] = sums.reshape(shares.shape)

    def add(index, total):
        return total + src[index].astype(jnp.float32) * source_area_ref[pl.ds(index, 1), :]

    zero = jnp.zeros((columns, block), jnp.float32)
    source = lanes_of(lax.fori_loop(0, src.shape[0], add, zero, unroll=8))

    def weigh(peer, held, total):
        share = shares[peer]
        for slot in range(capacity):
            total = total + held[peer, slot].astype(jnp.float32) * share[slot : slot + 1]
        return total

    total = weigh(me, outbound, zero)
    for step, (down, across) in enumerate(steps):
        blocks(step).wait_recv()
        from_row, from_col = lax.rem(row + n // cols - down, n // cols), lax.rem(col + cols - across, cols)
        total = weigh(from_row * cols + from_col, inbound_ref, total)
    rows = lax.broadcasted_iota(jnp.int32, own.shape, 0)
    own[...] = jnp.where(rows == 0, source, lanes_of(total))

    def masses(step):
        peer = lax.rem(me + step, n)
        return pltpu.make_async_remote_copy(
            src_ref=own,
            dst_ref=seen.at[step],
            send_sem=mass_send.at[step],
            recv_sem=mass_recv.at[step],
            device_id=(peer // cols, lax.rem(peer, cols)),
            device_id_type=MESH,
        )

    def tell(step, carry):
        masses(step).start()
        return carry

    def collect(step, total):
        masses(step).wait()
        return total + seen[step]

    lax.fori_loop(1, n, tell, 0)
    total = lax.fori_loop(1, n, collect, own[...])
    ratio = jnp.broadcast_to(total[0:1] / total[1:2], (columns, block))
    diagonal = lax.broadcasted_iota(jnp.int32, ratio.shape, 0) == lax.broadcasted_iota(jnp.int32, ratio.shape, 1)
    scale_ref[...] = jnp.broadcast_to(jnp.sum(jnp.where(diagonal, ratio, 0.0), axis=1, keepdims=True), ratio.shape)
    keep.wait()

    for step in range(n - 1):
        blocks(step).wait_send()


def order(rows, cols):
    count = rows * cols
    stride = next(k for k in (13, 11, 9, 7, 5, 3, 1) if math.gcd(k, count) == 1)
    return [divmod(stride * step % count, cols) for step in range(1, count)]


def exchange(n, cols, send_rows, pair_slot, pair_target, source_area, target_area, src_field, weights):
    columns, cells = src_field.shape
    block = source_area.shape[1]
    capacity = send_rows.shape[0]
    pairs = weights.shape[0]
    vmem = pl.BlockSpec(memory_space=pltpu.VMEM)
    smem = pl.BlockSpec(memory_space=pltpu.SMEM)
    hbm = pl.BlockSpec(memory_space=pl.ANY)
    return pl.pallas_call(
        functools.partial(exchange_kernel, n, cols),
        out_shape=(
            jax.ShapeDtypeStruct((n, capacity, columns, block), jnp.bfloat16),
            jax.ShapeDtypeStruct((columns, block), jnp.float32),
        ),
        in_specs=[smem, smem, smem, vmem, vmem, vmem, hbm, hbm],
        out_specs=(vmem, vmem),
        scratch_shapes=[
            pltpu.VMEM((cells // block, columns, block), jnp.bfloat16),
            pltpu.VMEM((n, capacity, columns, block), jnp.bfloat16),
            pltpu.VMEM(weights.shape, jnp.bfloat16),
            pltpu.VMEM((pairs, block), jnp.float32),
            pltpu.VMEM((n, 8, block), jnp.float32),
            pltpu.VMEM((8, block), jnp.float32),
            pltpu.VMEM((n, 8, block), jnp.float32),
            pltpu.SemaphoreType.DMA,
            pltpu.SemaphoreType.DMA((4,)),
            pltpu.SemaphoreType.DMA,
        ]
        + [pltpu.SemaphoreType.DMA((n,))] * 4,
        compiler_params=pltpu.CompilerParams(collective_id=0, has_side_effects=True),
        name="exchange",
    )(send_rows, pair_slot, pair_target, pair_slot, source_area, target_area, src_field, weights)


def regrid_kernel(lag, slot_ref, target_ref, inbound_ref, scale_ref, weight_ref, out_ref):
    step = pl.program_id(0)
    group, block = weight_ref.shape[:2]
    products = {}

    @pl.when(step == 0)
    def _():
        out_ref[...] = jnp.zeros_like(out_ref)

    def cells_of(target):
        return pl.ds(pl.multiple_of(target * block, block), block)

    for inner in range(group + lag):
        if inner < group:
            slot = slot_ref[step * group + inner]
            products[inner] = jnp.dot(inbound_ref[slot], weight_ref[inner], preferred_element_type=jnp.float32)
        if inner >= lag:
            cells = cells_of(target_ref[step * group + inner - lag])
            out_ref[:, cells] += products.pop(inner - lag)

    @pl.when(step == pl.num_programs(0) - 1)
    def _():
        def fix(index, carry):
            out_ref[:, cells_of(index)] = out_ref[:, cells_of(index)] * scale_ref[...]
            return carry

        lax.fori_loop(0, out_ref.shape[1] // block, fix, 0, unroll=8)


def regrid(inbound, scale, weights, pair_slot, pair_target, targets):
    slots, columns, block = inbound.shape
    pairs = weights.shape[0]
    group = next(g for g in (192, 96, 64, 48, 32, 16, 8, 4, 2, 1) if pairs % g == 0)
    whole = lambda *shape: pl.BlockSpec(shape, lambda i, *_: (0,) * len(shape))
    return pl.pallas_call(
        functools.partial(regrid_kernel, 6),
        out_shape=jax.ShapeDtypeStruct((columns, targets * block), jnp.float32),
        grid_spec=pltpu.PrefetchScalarGridSpec(
            num_scalar_prefetch=2,
            grid=(pairs // group,),
            in_specs=[
                whole(slots, columns, block),
                whole(columns, block),
                pl.BlockSpec((group, block, block), lambda i, *_: (i, 0, 0)),
            ],
            out_specs=whole(columns, targets * block),
        ),
        name="regrid",
    )(pair_slot, pair_target, inbound, scale, weights)


def shards(n, cols, src_field, src_area, tgt_area, weights, send_index, pair_slot, pair_target):
    columns, cell_count = src_field.shape
    block = weights.shape[1]
    targets = tgt_area.shape[0] // block
    inbound, scale = exchange(
        n, cols, send_index[0].T, pair_slot, pair_target,
        src_area.reshape(-1, block), tgt_area.reshape(targets, 1, block), src_field, weights,
    )
    return regrid(inbound.reshape(-1, columns, block), scale, weights, pair_slot, pair_target, targets)


def solution(mesh):
    rows, cols = mesh.shape["row"], mesh.shape["col"]
    in_specs = (
        P(None, ("row", "col")),
        P(("row", "col")),
        P(("row", "col")),
        P(("row", "col"), None, None),
        P(("row", "col"), None, None),
        P(("row", "col")),
        P(("row", "col")),
    )
    out_specs = P(None, ("row", "col"))
    body = functools.partial(shards, rows * cols, cols)
    return jax.shard_map(body, mesh=mesh, in_specs=in_specs, out_specs=out_specs, check_vma=False)
```
